8 devices in a mesh: dp: 1 (over z), sp: 8 (over y, x, core).
Axes of the slice: x: 2, y: 2, z: 1, core: 2. Of those that a mesh axis runs over, the one named last changes fastest.
Arguments:
- hidden: bfloat16 [6144, 5120], P(('dp', 'sp'))
- pos_ids: int32 [3, 6144], P(None, ('dp', 'sp'))
- cu_doc: int32 [3], P('dp')
- grad_y: bfloat16 [6144, 5120], P(('dp', 'sp'))
- norm_w: bfloat16 [5120], replicated
- w_q: bfloat16 [5120, 5120], replicated
- b_q: bfloat16 [5120], replicated
- w_k: bfloat16 [5120, 1024], replicated
- b_k: bfloat16 [1024], replicated
- w_v: bfloat16 [5120, 1024], replicated
- b_v: bfloat16 [1024], replicated
- w_o: bfloat16 [5120, 5120], replicated
Outputs:
- output 1: bfloat16 [6144, 5120], P(('dp', 'sp'))
- output 2: bfloat16 [6144, 5120], P(('dp', 'sp'))
- output 3: float32 [5120], P(('dp', 'sp'))
- output 4: float32 [5120, 5120], P(('dp', 'sp'))
- output 5: float32 [5120], P(('dp', 'sp'))
- output 6: float32 [5120, 1024], P(('dp', 'sp'))
- output 7: float32 [1024], P(('dp', 'sp'))
- output 8: float32 [5120, 1024], P(('dp', 'sp'))
- output 9: float32 [1024], P(('dp', 'sp'))
- output 10: float32 [5120, 5120], P(('dp', 'sp'))
All inputs are finite; a program needn't handle non-finite values.
Results may differ from the reference program's by a relative error of at most 0.015078.
Values are sent between devices in bfloat16 or wider.
A program may use at most 1 GiB of HBM per device.

```python
import math
import jax
import jax.numpy as jnp
from jax import lax

HIDDEN = 5120
QUERY_HEADS = 40
KEY_HEADS = 8
GROUP_SIZE = 8
SHARD_LEN = 768
NUM_DOCS = 2
HEAD_DIM = 128
SECTION_ONE = 16
SECTION_TWO = 40
ROW_BUDGET = 4096
SEQ_LEN = GROUP_SIZE * SHARD_LEN
Q_WIDTH = QUERY_HEADS * HEAD_DIM
KV_WIDTH = KEY_HEADS * HEAD_DIM
ROPE_BASE = 1000000.0
NORM_EPS = 1e-6


def draw_layout(layout_key):
    cut_key, off_key, width_key = jax.random.split(layout_key, 3)
    inner_len = SHARD_LEN - 1
    cand_idx = jax.random.permutation(cut_key, GROUP_SIZE * inner_len)[: NUM_DOCS - 1]
    cut_pos = jnp.sort((cand_idx // inner_len) * SHARD_LEN + cand_idx % inner_len + 1).astype(jnp.int32)
    cu_doc = jnp.concatenate([jnp.zeros((1,), jnp.int32), cut_pos, jnp.full((1,), SEQ_LEN, jnp.int32)])
    tok_idx = jnp.arange(SEQ_LEN, dtype=jnp.int32)
    doc_of = jnp.sum((cu_doc[None, 1:NUM_DOCS] <= tok_idx[:, None]).astype(jnp.int32), axis=1)
    doc_len = cu_doc[1:] - cu_doc[:-1]
    img_off = jax.random.randint(off_key, (NUM_DOCS,), 0, 1048576) % (doc_len // 4 + 1)
    img_wid = jax.random.randint(width_key, (NUM_DOCS,), 2, 17)
    img_hgt = jnp.maximum(1, (doc_len // 2) // img_wid)
    local_idx = tok_idx - cu_doc[doc_of]
    tok_off = img_off[doc_of]
    tok_wid = img_wid[doc_of]
    tok_hgt = img_hgt[doc_of]
    img_len = tok_wid * tok_hgt
    in_image = (local_idx >= tok_off) & (local_idx < tok_off + img_len)
    rel_idx = jnp.maximum(local_idx - tok_off, 0)
    text_pos = jnp.where(local_idx < tok_off, local_idx, local_idx - img_len + jnp.maximum(tok_wid, tok_hgt))
    pos_t = jnp.where(in_image, tok_off, text_pos)
    pos_h = jnp.where(in_image, tok_off + rel_idx // tok_wid, text_pos)
    pos_w = jnp.where(in_image, tok_off + rel_idx % tok_wid, text_pos)
    return cu_doc, jnp.stack([pos_t, pos_h, pos_w]).astype(jnp.int32)


def setup_inputs(seed: int = 0, part: int = 0) -> dict:
    part_keys = jax.random.split(jax.random.fold_in(jax.random.key(seed), part), 3)
    w_keys = jax.random.split(jax.random.key(seed + 1), 8)
    cu_doc, pos_ids = draw_layout(part_keys[2])
    hidden = jax.random.normal(part_keys[0], (SEQ_LEN, HIDDEN), jnp.float32).astype(jnp.bfloat16)
    grad_y = jax.random.normal(part_keys[1], (SEQ_LEN, HIDDEN), jnp.float32).astype(jnp.bfloat16)
    norm_w = (1.0 + 0.3 * jax.random.normal(w_keys[0], (HIDDEN,), jnp.float32)).astype(jnp.bfloat16)
    w_q = (jax.random.normal(w_keys[1], (HIDDEN, Q_WIDTH), jnp.float32) / math.sqrt(HIDDEN)).astype(jnp.bfloat16)
    b_q = (0.5 * jax.random.normal(w_keys[2], (Q_WIDTH,), jnp.float32)).astype(jnp.bfloat16)
    w_k = (jax.random.normal(w_keys[3], (HIDDEN, KV_WIDTH), jnp.float32) / math.sqrt(HIDDEN)).astype(jnp.bfloat16)
    b_k = (0.5 * jax.random.normal(w_keys[4], (KV_WIDTH,), jnp.float32)).astype(jnp.bfloat16)
    w_v = (jax.random.normal(w_keys[5], (HIDDEN, KV_WIDTH), jnp.float32) / math.sqrt(HIDDEN)).astype(jnp.bfloat16)
    b_v = (0.5 * jax.random.normal(w_keys[6], (KV_WIDTH,), jnp.float32)).astype(jnp.bfloat16)
    w_o = (jax.random.normal(w_keys[7], (Q_WIDTH, HIDDEN), jnp.float32) / math.sqrt(Q_WIDTH)).astype(jnp.bfloat16)
    return {"hidden": hidden, "pos_ids": pos_ids, "cu_doc": cu_doc, "grad_y": grad_y, "norm_w": norm_w, "w_q": w_q, "b_q": b_q, "w_k": w_k, "b_k": b_k, "w_v": w_v, "b_v": b_v, "w_o": w_o}


def rope_tables(pos_ids):
    freq_idx = jnp.arange(HEAD_DIM // 2)
    inv_freq = 1.0 / jnp.power(ROPE_BASE, jnp.arange(0, HEAD_DIM, 2).astype(jnp.float32) / HEAD_DIM)
    pos_f = pos_ids.astype(jnp.float32)
    chosen = jnp.where(freq_idx[None, :] < SECTION_ONE, pos_f[0][:, None], jnp.where(freq_idx[None, :] < SECTION_TWO, pos_f[1][:, None], pos_f[2][:, None]))
    angles = chosen * inv_freq[None, :]
    angles = jnp.concatenate([angles, angles], axis=-1)
    return jnp.cos(angles), jnp.sin(angles)


def rotate(values, cos_t, sin_t):
    half_dim = values.shape[-1] // 2
    turned = jnp.concatenate([-values[..., half_dim:], values[..., :half_dim]], axis=-1)
    return values * cos_t[:, None, :] + turned * sin_t[:, None, :]


def unrotate(grad_in, cos_t, sin_t):
    half_dim = grad_in.shape[-1] // 2
    scaled = grad_in * sin_t[:, None, :]
    turned = jnp.concatenate([scaled[..., half_dim:], -scaled[..., :half_dim]], axis=-1)
    return grad_in * cos_t[:, None, :] + turned


def doc_starts(cu_doc, tok_idx):
    bounds = cu_doc[:-1]
    return jnp.max(jnp.where(bounds[None, :] <= tok_idx[:, None], bounds[None, :], 0), axis=1)


def attend(q_grp, k_all, v_all, do_grp, starts):
    n_query, groups, grp_ratio, head_dim = q_grp.shape
    key_len = k_all.shape[0]
    row_cap = max(1, ROW_BUDGET // (groups * grp_ratio))
    block_len = math.gcd(n_query, 1 << (row_cap.bit_length() - 1))
    n_blocks = n_query // block_len
    qk_scale = 1.0 / math.sqrt(head_dim)
    key_idx = jnp.arange(key_len)
    k_f = k_all.astype(jnp.float32)
    v_f = v_all.astype(jnp.float32)

    def block_step(acc_pair, block_in):
        dk_acc, dv_acc = acc_pair
        q_blk, do_blk, start_blk, blk_idx = block_in
        q_f = q_blk.astype(jnp.float32)
        do_f = do_blk.astype(jnp.float32)
        q_idx = blk_idx * block_len + jnp.arange(block_len)
        allowed = (key_idx[None, :] <= q_idx[:, None]) & (key_idx[None, :] >= start_blk[:, None])
        scores = jnp.einsum("qgre,kge->gqrk", q_f, k_f) * qk_scale
        scores = jnp.where(allowed[None, :, None, :], scores, -1e30)
        prob_f = jax.nn.softmax(scores, axis=-1)
        prob_r = prob_f.astype(jnp.bfloat16).astype(jnp.float32)
        out_blk = jnp.einsum("gqrk,kge->qgre", prob_r, v_f).astype(jnp.bfloat16)
        d_prob = jnp.einsum("qgre,kge->gqrk", do_f, v_f)
        row_delta = jnp.sum(prob_f * d_prob, axis=-1, keepdims=True)
        d_score = (prob_f * (d_prob - row_delta) * qk_scale).astype(jnp.bfloat16).astype(jnp.float32)
        dq_blk = jnp.einsum("gqrk,kge->qgre", d_score, k_f).astype(jnp.bfloat16)
        dk_acc = dk_acc + jnp.einsum("gqrk,qgre->kge", d_score, q_f)
        dv_acc = dv_acc + jnp.einsum("gqrk,qgre->kge", prob_r, do_f)
        return (dk_acc, dv_acc), (out_blk, dq_blk)

    blocks_in = (q_grp.reshape(n_blocks, block_len, groups, grp_ratio, head_dim), do_grp.reshape(n_blocks, block_len, groups, grp_ratio, head_dim), starts.reshape(n_blocks, block_len), jnp.arange(n_blocks))
    zero_acc = jnp.zeros((key_len, groups, head_dim), jnp.float32)
    acc_pair, outs_pair = lax.scan(block_step, (zero_acc, zero_acc), blocks_in)
    return outs_pair[0].reshape(q_grp.shape), outs_pair[1].reshape(q_grp.shape), acc_pair[0], acc_pair[1]


def reference(hidden, pos_ids, cu_doc, grad_y, norm_w, w_q, b_q, w_k, b_k, w_v, b_v, w_o):
    grp_ratio = QUERY_HEADS // KEY_HEADS
    h_f32 = hidden.astype(jnp.float32)
    inv_rms = lax.rsqrt(jnp.mean(h_f32 * h_f32, axis=-1, keepdims=True) + NORM_EPS)
    normed = h_f32 * inv_rms
    gain = norm_w.astype(jnp.float32)
    normed_b = (normed * gain).astype(jnp.bfloat16)
    cos_t, sin_t = rope_tables(pos_ids)
    q_lin = jnp.dot(normed_b, w_q, preferred_element_type=jnp.float32) + b_q.astype(jnp.float32)
    k_lin = jnp.dot(normed_b, w_k, preferred_element_type=jnp.float32) + b_k.astype(jnp.float32)
    q_rot = rotate(q_lin.reshape(SEQ_LEN, QUERY_HEADS, HEAD_DIM), cos_t, sin_t).astype(jnp.bfloat16)
    k_rot = rotate(k_lin.reshape(SEQ_LEN, KEY_HEADS, HEAD_DIM), cos_t, sin_t).astype(jnp.bfloat16)
    v_val = (jnp.dot(normed_b, w_v, preferred_element_type=jnp.float32) + b_v.astype(jnp.float32)).astype(jnp.bfloat16).reshape(SEQ_LEN, KEY_HEADS, HEAD_DIM)
    d_attn = jnp.dot(grad_y, w_o.T, preferred_element_type=jnp.float32).astype(jnp.bfloat16)
    starts = doc_starts(cu_doc, jnp.arange(SEQ_LEN))
    out_b, dq_b, dk_acc, dv_acc = attend(q_rot.reshape(SEQ_LEN, KEY_HEADS, grp_ratio, HEAD_DIM), k_rot, v_val, d_attn.reshape(SEQ_LEN, KEY_HEADS, grp_ratio, HEAD_DIM), starts)
    attn_out = out_b.reshape(SEQ_LEN, Q_WIDTH)
    y_out = (h_f32 + jnp.dot(attn_out, w_o, preferred_element_type=jnp.float32)).astype(jnp.bfloat16)
    grad_w_o = jnp.dot(attn_out.T, grad_y, preferred_element_type=jnp.float32)
    dq_lin = unrotate(dq_b.reshape(SEQ_LEN, QUERY_HEADS, HEAD_DIM).astype(jnp.float32), cos_t, sin_t).reshape(SEQ_LEN, Q_WIDTH)
    dk_lin = unrotate(dk_acc.astype(jnp.bfloat16).astype(jnp.float32), cos_t, sin_t).reshape(SEQ_LEN, KV_WIDTH)
    dv_lin = dv_acc.astype(jnp.bfloat16).reshape(SEQ_LEN, KV_WIDTH)
    dq_b16 = dq_lin.astype(jnp.bfloat16)
    dk_b16 = dk_lin.astype(jnp.bfloat16)
    grad_b_q = jnp.sum(dq_lin, axis=0)
    grad_b_k = jnp.sum(dk_lin, axis=0)
    grad_b_v = jnp.sum(dv_lin.astype(jnp.float32), axis=0)
    grad_w_q = jnp.dot(normed_b.T, dq_b16, preferred_element_type=jnp.float32)
    grad_w_k = jnp.dot(normed_b.T, dk_b16, preferred_element_type=jnp.float32)
    grad_w_v = jnp.dot(normed_b.T, dv_lin, preferred_element_type=jnp.float32)
    d_norm = jnp.dot(dq_b16, w_q.T, preferred_element_type=jnp.float32) + jnp.dot(dk_b16, w_k.T, preferred_element_type=jnp.float32) + jnp.dot(dv_lin, w_v.T, preferred_element_type=jnp.float32)
    grad_norm_w = jnp.sum(d_norm * normed, axis=0)
    d_scaled = d_norm * gain
    d_hidden = inv_rms * (d_scaled - normed * jnp.mean(d_scaled * normed, axis=-1, keepdims=True))
    grad_hidden = (grad_y.astype(jnp.float32) + d_hidden).astype(jnp.bfloat16)
    return (y_out, grad_hidden, grad_norm_w, grad_w_q, grad_b_q, grad_w_k, grad_b_k, grad_w_v, grad_b_v, grad_w_o)
```

```python
import functools
import math
import jax
import jax.numpy as jnp
from jax import lax
from jax.experimental import pallas as pl
from jax.experimental.pallas import tpu as pltpu
from jax.sharding import PartitionSpec as P

HEAD_DIM = 128
SECTION_ONE = 16
SECTION_TWO = 40
ROPE_BASE = 1000000.0
NORM_EPS = 1e-6
LOG2E = 1.4426950408889634
NEG = -1e30
F32 = jnp.float32
BF16 = jnp.bfloat16


def rope_tables(pos_ids):
    freq_idx = jnp.arange(HEAD_DIM) % (HEAD_DIM // 2)
    exponent = 2 * freq_idx.astype(F32) / HEAD_DIM
    inv_freq = 1.0 / jnp.power(ROPE_BASE, exponent)
    pos_f = pos_ids.astype(F32)
    chosen = jnp.where(freq_idx[None, :] < SECTION_ONE, pos_f[0][:, None], jnp.where(freq_idx[None, :] < SECTION_TWO, pos_f[1][:, None], pos_f[2][:, None]))
    angles = chosen * inv_freq[None, :]
    sign = jnp.where(jnp.arange(HEAD_DIM) < HEAD_DIM // 2, -1.0, 1.0).astype(F32)
    return jnp.cos(angles), jnp.sin(angles) * sign[None, :]


def dot(a, b):
    return lax.dot_general(a, b, (((1,), (0,)), ((), ())), preferred_element_type=F32)


def dot_t(a, b):
    return lax.dot_general(a, b, (((1,), (1,)), ((), ())), preferred_element_type=F32)


def qkv_kernel(n_rot, u_ref, w_ref, b_ref, cos_ref, sin_ref, out_ref):
    lin = dot(u_ref[...], w_ref[...]) + b_ref[...]
    cos_t = cos_ref[...]
    sin_t = sin_ref[...]
    for idx in range(n_rot):
        cols = slice(idx * HEAD_DIM, (idx + 1) * HEAD_DIM)
        part = lin[:, cols]
        out_ref[:, cols] = (part * cos_t + pltpu.roll(part, HEAD_DIM // 2, 1) * sin_t).astype(BF16)
    out_ref[:, n_rot * HEAD_DIM:] = lin[:, n_rot * HEAD_DIM:].astype(BF16)


def project(u_all, w_cat, b_cat, cos_t, sin_t, n_rot):
    tokens, hidden = u_all.shape
    width = w_cat.shape[1]
    rows = math.gcd(tokens, 512)
    return pl.pallas_call(
        functools.partial(qkv_kernel, n_rot),
        out_shape=jax.ShapeDtypeStruct((tokens, width), BF16),
        grid=(tokens // rows,),
        in_specs=[
            pl.BlockSpec((rows, hidden), lambda i: (i, 0)),
            pl.BlockSpec((hidden, width), lambda i: (0, 0), pipeline_mode=pl.Buffered(1)),
            pl.BlockSpec((1, width), lambda i: (0, 0)),
            pl.BlockSpec((rows, HEAD_DIM), lambda i: (i, 0)),
            pl.BlockSpec((rows, HEAD_DIM), lambda i: (i, 0)),
        ],
        out_specs=pl.BlockSpec((rows, width), lambda i: (i, 0)),
        compiler_params=pltpu.CompilerParams(vmem_limit_bytes=60 * 1024 * 1024),
        cost_estimate=pl.CostEstimate(flops=2 * tokens * hidden * width, bytes_accessed=2 * (tokens * hidden + hidden * width + tokens * width), transcendentals=0),
        name="qkv_rope",
    )(u_all, w_cat, b_cat, cos_t, sin_t)


def attn_kernel(blk, n_heads, n_blk, cu_ref, q_ref, do_ref, k_ref, v_ref, cos_ref, sin_ref,
                o_ref, gq_ref, gk_ref, gv_ref, gbq_ref, gbk_ref, gbv_ref,
                s_scr, dp_scr, dk_scr, dv_scr, kt_scr, vt_scr):
    head = pl.program_id(0)
    row_blk = pl.program_id(1)
    half = HEAD_DIM // 2
    scale = 1.0 / math.sqrt(HEAD_DIM)
    cut = cu_ref[1]
    row_0 = row_blk * blk

    @pl.when((head == 0) & (row_blk == 0))
    def _():
        @pl.loop(0, n_blk)
        def _(c):
            rows = pl.ds(pl.multiple_of(c * blk, blk), blk)
            kt_scr[c] = k_ref[rows, :].T
            vt_scr[c] = v_ref[rows, :].T
            dk_scr[c] = jnp.zeros((blk, HEAD_DIM), F32)
            dv_scr[c] = jnp.zeros((blk, HEAD_DIM), F32)

    first_tok = jnp.where(row_0 >= cut, cut, 0)
    lo = first_tok // blk
    hi = row_blk + 1
    straddle = (row_0 < cut) & (cut < row_0 + blk)
    ragged = lo * blk < first_tok

    q_blk = q_ref[...]
    do_blk = do_ref[...]

    def scores(c, m_acc, masked):
        rows = pl.ds(pl.multiple_of(c * blk, blk), blk)
        s_t = dot_t(k_ref[rows, :], q_blk)
        if masked:
            key_idx = c * blk + lax.broadcasted_iota(jnp.int32, (blk, blk), 0)
            q_idx = row_0 + lax.broadcasted_iota(jnp.int32, (blk, blk), 1)
            start = jnp.where(q_idx >= cut, cut, 0)
            s_t = jnp.where((key_idx <= q_idx) & (key_idx >= start), s_t, NEG)
        s_scr[c] = s_t
        dp_scr[c] = dot_t(v_ref[rows, :], do_blk)
        return jnp.maximum(m_acc, jnp.max(s_t.reshape(blk // 8, 8, blk), axis=0))

    def phase_a(c, m_acc):
        need = (c == row_blk) | straddle | ((c == lo) & ragged)
        return lax.cond(need, lambda m: scores(c, m, True), lambda m: scores(c, m, False), m_acc)

    m_acc = lax.fori_loop(lo, hi, phase_a, jnp.full((8, blk), NEG, F32))
    m_row = jnp.max(m_acc, axis=0, keepdims=True) * (scale * LOG2E)

    def phase_b(c, accs):
        l_acc, d_acc = accs
        p = jnp.exp2(s_scr[c] * (scale * LOG2E) - m_row)
        s_scr[c] = p
        pd = p * dp_scr[c]
        return (l_acc + jnp.sum(p.reshape(blk // 8, 8, blk), axis=0), d_acc + jnp.sum(pd.reshape(blk // 8, 8, blk), axis=0))

    zero_8 = jnp.zeros((8, blk), F32)
    l_acc, d_acc = lax.fori_loop(lo, hi, phase_b, (zero_8, zero_8))
    inv_l = 1.0 / jnp.sum(l_acc, axis=0, keepdims=True)
    delta = jnp.sum(d_acc, axis=0, keepdims=True) * inv_l

    def phase_c(c, accs):
        o_acc, dq_acc = accs
        p = s_scr[c] * inv_l
        p_b = p.astype(BF16)
        ds_b = (p * (dp_scr[c] - delta) * scale).astype(BF16)
        o_acc = o_acc + dot(vt_scr[c], p_b)
        dq_acc = dq_acc + dot(kt_scr[c], ds_b)
        dk_scr[c] += dot(ds_b, q_blk)
        dv_scr[c] += dot(p_b, do_blk)
        return o_acc, dq_acc

    zero_t = jnp.zeros((HEAD_DIM, blk), F32)
    o_acc, dq_acc = lax.fori_loop(lo, hi, phase_c, (zero_t, zero_t))
    o_ref[...] = o_acc.T.astype(BF16)

    def unrotate(grad, rows):
        return grad * cos_ref[rows, :] + pltpu.roll(grad * sin_ref[rows, :], half, 1)

    dq = dq_acc.T.astype(BF16).astype(F32)
    gq = unrotate(dq, pl.ds(pl.multiple_of(row_0, blk), blk))
    gq_ref[...] = gq.astype(BF16)

    @pl.when(row_blk == 0)
    def _():
        gbq_ref[...] = jnp.zeros_like(gbq_ref)

    gbq_ref[...] += jnp.sum(gq.reshape(blk // 8, 8, HEAD_DIM), axis=0)

    @pl.when((head == n_heads - 1) & (row_blk == n_blk - 1))
    def _():
        gbk_ref[...] = jnp.zeros_like(gbk_ref)
        gbv_ref[...] = jnp.zeros_like(gbv_ref)

        @pl.loop(0, n_blk)
        def _(c):
            rows = pl.ds(pl.multiple_of(c * blk, blk), blk)
            gk = unrotate(dk_scr[c].astype(BF16).astype(F32), rows)
            gk_ref[rows, :] = gk.astype(BF16)
            gbk_ref[...] += jnp.sum(gk.reshape(blk // 8, 8, HEAD_DIM), axis=0)
            gv = dv_scr[c].astype(BF16)
            gv_ref[rows, :] = gv
            gbv_ref[...] += jnp.sum(gv.astype(F32).reshape(blk // 8, 8, HEAD_DIM), axis=0)


def attend(cu_doc, qkv, d_out, cos_t, sin_t, n_heads):
    tokens = qkv.shape[0]
    blk = math.gcd(tokens, 512)
    n_blk = tokens // blk
    whole = functools.partial(pl.BlockSpec, pipeline_mode=pl.Buffered(1))
    width = n_heads * HEAD_DIM
    head_blk = pl.BlockSpec((blk, HEAD_DIM), lambda h, i, cu: (i, h))
    return pl.pallas_call(
        functools.partial(attn_kernel, blk, n_heads, n_blk),
        out_shape=[
            jax.ShapeDtypeStruct((tokens, width), BF16),
            jax.ShapeDtypeStruct((tokens, width), BF16),
            jax.ShapeDtypeStruct((tokens, HEAD_DIM), BF16),
            jax.ShapeDtypeStruct((tokens, HEAD_DIM), BF16),
            jax.ShapeDtypeStruct((8, width), F32),
            jax.ShapeDtypeStruct((8, HEAD_DIM), F32),
            jax.ShapeDtypeStruct((8, HEAD_DIM), F32),
        ],
        grid_spec=pltpu.PrefetchScalarGridSpec(
            num_scalar_prefetch=1,
            grid=(n_heads, n_blk),
            in_specs=[
                head_blk,
                head_blk,
                whole((tokens, HEAD_DIM), lambda h, i, cu: (0, n_heads)),
                whole((tokens, HEAD_DIM), lambda h, i, cu: (0, n_heads + 1)),
                whole((tokens, HEAD_DIM), lambda h, i, cu: (0, 0)),
                whole((tokens, HEAD_DIM), lambda h, i, cu: (0, 0)),
            ],
            out_specs=[
                head_blk,
                head_blk,
                pl.BlockSpec((tokens, HEAD_DIM), lambda h, i, cu: (0, 0)),
                pl.BlockSpec((tokens, HEAD_DIM), lambda h, i, cu: (0, 0)),
                pl.BlockSpec((8, HEAD_DIM), lambda h, i, cu: (0, h)),
                pl.BlockSpec((8, HEAD_DIM), lambda h, i, cu: (0, 0)),
                pl.BlockSpec((8, HEAD_DIM), lambda h, i, cu: (0, 0)),
            ],
            scratch_shapes=[
                pltpu.VMEM((n_blk, blk, blk), F32),
                pltpu.VMEM((n_blk, blk, blk), F32),
                pltpu.VMEM((n_blk, blk, HEAD_DIM), F32),
                pltpu.VMEM((n_blk, blk, HEAD_DIM), F32),
                pltpu.VMEM((n_blk, HEAD_DIM, blk), BF16),
                pltpu.VMEM((n_blk, HEAD_DIM, blk), BF16),
            ],
        ),
        compiler_params=pltpu.CompilerParams(vmem_limit_bytes=63 * 1024 * 1024),
        cost_estimate=pl.CostEstimate(flops=6 * n_heads * tokens * tokens * HEAD_DIM * 2, bytes_accessed=10 * tokens * width, transcendentals=0),
        name="attn_fwd_bwd",
    )(cu_doc, qkv, d_out, qkv, qkv, cos_t, sin_t)


def solution(mesh):
    n_dev = mesh.shape["sp"]
    tok_spec = P(("dp", "sp"), None)
    vec_spec = P(("dp", "sp"))
    rep_spec = P()

    def exchange(parts):
        return lax.all_to_all(parts, "sp", 0, 0, tiled=True)

    def per_device(hidden, pos_ids, cu_doc, grad_y, norm_w, w_q, b_q, w_k, b_k, w_v, b_v, w_o):
        tokens, width = hidden.shape
        me = lax.axis_index("sp")
        q_cols = w_q.shape[1] // n_dev
        kv_cols = w_k.shape[1] // n_dev
        n_heads = q_cols // HEAD_DIM

        h_f32 = hidden.astype(F32)
        inv_rms = lax.rsqrt(jnp.mean(h_f32 * h_f32, axis=-1, keepdims=True) + NORM_EPS)
        normed = h_f32 * inv_rms
        gain = norm_w.astype(F32)
        u_loc = (normed * gain).astype(BF16)
        u_all = lax.all_gather(u_loc, "sp", axis=0, tiled=True)
        pos_all = lax.all_gather(pos_ids, "sp", axis=1, tiled=True)
        cos_t, sin_t = rope_tables(pos_all)

        d_attn = jnp.einsum("td,qd->tq", grad_y, w_o, preferred_element_type=F32).astype(BF16)
        d_parts = d_attn.reshape(tokens, n_dev, q_cols).transpose(1, 0, 2)
        d_out = exchange(d_parts).reshape(n_dev * tokens, q_cols)

        def own(w, cols):
            return lax.dynamic_slice_in_dim(w, me * cols, cols, axis=w.ndim - 1)

        w_cat = jnp.concatenate([own(w_q, q_cols), own(w_k, kv_cols), own(w_v, kv_cols)], axis=1)
        b_cat = jnp.concatenate([own(b_q, q_cols), own(b_k, kv_cols), own(b_v, kv_cols)]).astype(F32)[None, :]
        qkv = project(u_all, w_cat, b_cat, cos_t, sin_t, n_heads + kv_cols // HEAD_DIM)

        gy_src, qkv = lax.optimization_barrier((grad_y, qkv))
        gy_all = lax.all_gather(gy_src, "sp", axis=0, tiled=True)

        o_h, gq_h, gk_h, gv_h, gbq, gbk, gbv = attend(cu_doc, qkv, d_out, cos_t, sin_t, n_heads)

        o_tok = exchange(o_h.reshape(n_dev, tokens, q_cols)).transpose(1, 0, 2).reshape(tokens, n_dev * q_cols)
        gq_tok = exchange(gq_h.reshape(n_dev, tokens, q_cols)).transpose(1, 0, 2).reshape(tokens, n_dev * q_cols)
        gkv_h = jnp.stack([gk_h.reshape(n_dev, tokens, kv_cols), gv_h.reshape(n_dev, tokens, kv_cols)], axis=1)
        gkv_tok = exchange(gkv_h).transpose(1, 2, 0, 3).reshape(2, tokens, n_dev * kv_cols)

        grad_w_o = lax.dot_general(o_h, gy_all, (((0,), (0,)), ((), ())), preferred_element_type=F32)
        g_cat = jnp.concatenate([gq_h, gk_h, gv_h], axis=1)
        gw_cat = lax.dot_general(u_all, g_cat, (((0,), (0,)), ((), ())), preferred_element_type=F32)
        rows = width // n_dev
        gw_got = exchange(gw_cat.reshape(n_dev, rows, q_cols + 2 * kv_cols))

        def columns(lo, size):
            return gw_got[:, :, lo:lo + size].transpose(1, 0, 2).reshape(rows, n_dev * size)

        grad_w_q = columns(0, q_cols)
        grad_w_k = columns(q_cols, kv_cols)
        grad_w_v = columns(q_cols + kv_cols, kv_cols)

        y_out = (h_f32 + jnp.dot(o_tok, w_o, preferred_element_type=F32)).astype(BF16)
        d_norm = dot_t(gq_tok, w_q) + dot_t(gkv_tok[0], w_k) + dot_t(gkv_tok[1], w_v)
        grad_norm_w = lax.psum_scatter(jnp.sum(d_norm * normed, axis=0), "sp", scatter_dimension=0, tiled=True)
        d_scaled = d_norm * gain
        d_hidden = inv_rms * (d_scaled - normed * jnp.mean(d_scaled * normed, axis=-1, keepdims=True))
        grad_hidden = (grad_y.astype(F32) + d_hidden).astype(BF16)
        return (y_out, grad_hidden, grad_norm_w, grad_w_q, jnp.sum(gbq, axis=0), grad_w_k, jnp.sum(gbk, axis=0), grad_w_v, jnp.sum(gbv, axis=0), grad_w_o)

    in_specs = (tok_spec, P(None, ("dp", "sp")), P("dp"), tok_spec, rep_spec, rep_spec, rep_spec, rep_spec, rep_spec, rep_spec, rep_spec, rep_spec)
    out_specs = (tok_spec, tok_spec, vec_spec, tok_spec, vec_spec, tok_spec, vec_spec, tok_spec, vec_spec, tok_spec)
    return jax.shard_map(per_device, mesh=mesh, in_specs=in_specs, out_specs=out_specs, check_vma=False)
```

```python
import functools
import math
import jax
import jax.numpy as jnp
from jax import lax
from jax.experimental import pallas as pl
from jax.experimental.pallas import tpu as pltpu
from jax.sharding import PartitionSpec as P

HEAD_DIM = 128
SECTION_ONE = 16
SECTION_TWO = 40
ROPE_BASE = 1000000.0
NORM_EPS = 1e-6
LOG2E = 1.4426950408889634
NEG = -1e30
F32 = jnp.float32
BF16 = jnp.bfloat16


def rope_tables(pos_ids):
    freq_idx = jnp.arange(HEAD_DIM) % (HEAD_DIM // 2)
    exponent = 2 * freq_idx.astype(F32) / HEAD_DIM
    inv_freq = 1.0 / jnp.power(ROPE_BASE, exponent)
    pos_f = pos_ids.astype(F32)
    chosen = jnp.where(freq_idx[None, :] < SECTION_ONE, pos_f[0][:, None], jnp.where(freq_idx[None, :] < SECTION_TWO, pos_f[1][:, None], pos_f[2][:, None]))
    angles = chosen * inv_freq[None, :]
    sign = jnp.where(jnp.arange(HEAD_DIM) < HEAD_DIM // 2, -1.0, 1.0).astype(F32)
    return jnp.cos(angles), jnp.sin(angles) * sign[None, :]


def dot(a, b):
    return lax.dot_general(a, b, (((1,), (0,)), ((), ())), preferred_element_type=F32)


def dot_t(a, b):
    return lax.dot_general(a, b, (((1,), (1,)), ((), ())), preferred_element_type=F32)


def qkv_kernel(n_rot, u_ref, w_ref, b_ref, cos_ref, sin_ref, out_ref):
    lin = dot(u_ref[...], w_ref[...]) + b_ref[...]
    cos_t = cos_ref[...]
    sin_t = sin_ref[...]
    for idx in range(n_rot):
        cols = slice(idx * HEAD_DIM, (idx + 1) * HEAD_DIM)
        part = lin[:, cols]
        out_ref[:, cols] = (part * cos_t + pltpu.roll(part, HEAD_DIM // 2, 1) * sin_t).astype(BF16)
    out_ref[:, n_rot * HEAD_DIM:] = lin[:, n_rot * HEAD_DIM:].astype(BF16)


def project(u_all, w_cat, b_cat, cos_t, sin_t, n_rot):
    tokens, hidden = u_all.shape
    width = w_cat.shape[1]
    rows = math.gcd(tokens, 512)
    return pl.pallas_call(
        functools.partial(qkv_kernel, n_rot),
        out_shape=jax.ShapeDtypeStruct((tokens, width), BF16),
        grid=(tokens // rows,),
        in_specs=[
            pl.BlockSpec((rows, hidden), lambda i: (i, 0)),
            pl.BlockSpec((hidden, width), lambda i: (0, 0), pipeline_mode=pl.Buffered(1)),
            pl.BlockSpec((1, width), lambda i: (0, 0)),
            pl.BlockSpec((rows, HEAD_DIM), lambda i: (i, 0)),
            pl.BlockSpec((rows, HEAD_DIM), lambda i: (i, 0)),
        ],
        out_specs=pl.BlockSpec((rows, width), lambda i: (i, 0)),
        compiler_params=pltpu.CompilerParams(vmem_limit_bytes=60 * 1024 * 1024),
        cost_estimate=pl.CostEstimate(flops=2 * tokens * hidden * width, bytes_accessed=2 * (tokens * hidden + hidden * width + tokens * width), transcendentals=0),
        name="qkv_rope",
    )(u_all, w_cat, b_cat, cos_t, sin_t)


def attn_kernel(blk, n_heads, n_blk, cu_ref, q_ref, do_ref, k_ref, v_ref, cos_ref, sin_ref,
                o_ref, gq_ref, gk_ref, gv_ref, gbq_ref, gbk_ref, gbv_ref,
                s_scr, dp_scr, dk_scr, dv_scr, kt_scr, vt_scr):
    head = pl.program_id(0)
    row_blk = pl.program_id(1)
    half = HEAD_DIM // 2
    scale = 1.0 / math.sqrt(HEAD_DIM)
    cut = cu_ref[1]
    row_0 = row_blk * blk

    @pl.when((head == 0) & (row_blk == 0))
    def _():
        @pl.loop(0, n_blk)
        def _(c):
            rows = pl.ds(pl.multiple_of(c * blk, blk), blk)
            kt_scr[c] = k_ref[rows, :].T
            vt_scr[c] = v_ref[rows, :].T
            dk_scr[c] = jnp.zeros((blk, HEAD_DIM), F32)
            dv_scr[c] = jnp.zeros((blk, HEAD_DIM), F32)

    first_tok = jnp.where(row_0 >= cut, cut, 0)
    lo = first_tok // blk
    hi = row_blk + 1
    straddle = (row_0 < cut) & (cut < row_0 + blk)
    ragged = lo * blk < first_tok

    q_blk = q_ref[...]
    do_blk = do_ref[...]

    def scores(c, m_acc, masked):
        rows = pl.ds(pl.multiple_of(c * blk, blk), blk)
        s_t = dot_t(k_ref[rows, :], q_blk)
        if masked:
            key_idx = c * blk + lax.broadcasted_iota(jnp.int32, (blk, blk), 0)
            q_idx = row_0 + lax.broadcasted_iota(jnp.int32, (blk, blk), 1)
            start = jnp.where(q_idx >= cut, cut, 0)
            s_t = jnp.where((key_idx <= q_idx) & (key_idx >= start), s_t, NEG)
        s_scr[c] = s_t
        dp_scr[c] = dot_t(v_ref[rows, :], do_blk)
        return jnp.maximum(m_acc, jnp.max(s_t.reshape(blk // 8, 8, blk), axis=0))

    def phase_a(c, m_acc):
        need = (c == row_blk) | straddle | ((c == lo) & ragged)
        return lax.cond(need, lambda m: scores(c, m, True), lambda m: scores(c, m, False), m_acc)

    m_acc = lax.fori_loop(lo, hi, phase_a, jnp.full((8, blk), NEG, F32))
    m_row = jnp.max(m_acc, axis=0, keepdims=True) * (scale * LOG2E)

    def phase_b(c, accs):
        l_acc, d_acc = accs
        p = jnp.exp2(s_scr[c] * (scale * LOG2E) - m_row)
        s_scr[c] = p
        pd = p * dp_scr[c]
        return (l_acc + jnp.sum(p.reshape(blk // 8, 8, blk), axis=0), d_acc + jnp.sum(pd.reshape(blk // 8, 8, blk), axis=0))

    zero_8 = jnp.zeros((8, blk), F32)
    l_acc, d_acc = lax.fori_loop(lo, hi, phase_b, (zero_8, zero_8))
    inv_l = 1.0 / jnp.sum(l_acc, axis=0, keepdims=True)
    delta = jnp.sum(d_acc, axis=0, keepdims=True) * inv_l

    def phase_c(c, accs):
        o_acc, dq_acc = accs
        p = s_scr[c] * inv_l
        p_b = p.astype(BF16)
        ds_b = (p * (dp_scr[c] - delta) * scale).astype(BF16)
        o_acc = o_acc + dot(vt_scr[c], p_b)
        dq_acc = dq_acc + dot(kt_scr[c], ds_b)
        dk_scr[c] += dot(ds_b, q_blk)
        dv_scr[c] += dot(p_b, do_blk)
        return o_acc, dq_acc

    zero_t = jnp.zeros((HEAD_DIM, blk), F32)
    o_acc, dq_acc = lax.fori_loop(lo, hi, phase_c, (zero_t, zero_t))
    o_ref[...] = o_acc.T.astype(BF16)

    def unrotate(grad, rows):
        return grad * cos_ref[rows, :] + pltpu.roll(grad * sin_ref[rows, :], half, 1)

    dq = dq_acc.T.astype(BF16).astype(F32)
    gq = unrotate(dq, pl.ds(pl.multiple_of(row_0, blk), blk))
    gq_ref[...] = gq.astype(BF16)

    @pl.when(row_blk == 0)
    def _():
        gbq_ref[...] = jnp.zeros_like(gbq_ref)

    gbq_ref[...] += jnp.sum(gq.reshape(blk // 8, 8, HEAD_DIM), axis=0)

    @pl.when((head == n_heads - 1) & (row_blk == n_blk - 1))
    def _():
        gbk_ref[...] = jnp.zeros_like(gbk_ref)
        gbv_ref[...] = jnp.zeros_like(gbv_ref)

        @pl.loop(0, n_blk)
        def _(c):
            rows = pl.ds(pl.multiple_of(c * blk, blk), blk)
            gk = unrotate(dk_scr[c].astype(BF16).astype(F32), rows)
            gk_ref[rows, :] = gk.astype(BF16)
            gbk_ref[...] += jnp.sum(gk.reshape(blk // 8, 8, HEAD_DIM), axis=0)
            gv = dv_scr[c].astype(BF16)
            gv_ref[rows, :] = gv
            gbv_ref[...] += jnp.sum(gv.astype(F32).reshape(blk // 8, 8, HEAD_DIM), axis=0)


def attend(cu_doc, qkv, d_out, cos_t, sin_t, n_heads):
    tokens = qkv.shape[0]
    blk = math.gcd(tokens, 512)
    n_blk = tokens // blk
    whole = functools.partial(pl.BlockSpec, pipeline_mode=pl.Buffered(1))
    width = n_heads * HEAD_DIM
    head_blk = pl.BlockSpec((blk, HEAD_DIM), lambda h, i, cu: (i, h))
    return pl.pallas_call(
        functools.partial(attn_kernel, blk, n_heads, n_blk),
        out_shape=[
            jax.ShapeDtypeStruct((tokens, width), BF16),
            jax.ShapeDtypeStruct((tokens, width), BF16),
            jax.ShapeDtypeStruct((tokens, HEAD_DIM), BF16),
            jax.ShapeDtypeStruct((tokens, HEAD_DIM), BF16),
            jax.ShapeDtypeStruct((8, width), F32),
            jax.ShapeDtypeStruct((8, HEAD_DIM), F32),
            jax.ShapeDtypeStruct((8, HEAD_DIM), F32),
        ],
        grid_spec=pltpu.PrefetchScalarGridSpec(
            num_scalar_prefetch=1,
            grid=(n_heads, n_blk),
            in_specs=[
                head_blk,
                head_blk,
                whole((tokens, HEAD_DIM), lambda h, i, cu: (0, n_heads)),
                whole((tokens, HEAD_DIM), lambda h, i, cu: (0, n_heads + 1)),
                whole((tokens, HEAD_DIM), lambda h, i, cu: (0, 0)),
                whole((tokens, HEAD_DIM), lambda h, i, cu: (0, 0)),
            ],
            out_specs=[
                head_blk,
                head_blk,
                pl.BlockSpec((tokens, HEAD_DIM), lambda h, i, cu: (0, 0)),
                pl.BlockSpec((tokens, HEAD_DIM), lambda h, i, cu: (0, 0)),
                pl.BlockSpec((8, HEAD_DIM), lambda h, i, cu: (0, h)),
                pl.BlockSpec((8, HEAD_DIM), lambda h, i, cu: (0, 0)),
                pl.BlockSpec((8, HEAD_DIM), lambda h, i, cu: (0, 0)),
            ],
            scratch_shapes=[
                pltpu.VMEM((n_blk, blk, blk), F32),
                pltpu.VMEM((n_blk, blk, blk), F32),
                pltpu.VMEM((n_blk, blk, HEAD_DIM), F32),
                pltpu.VMEM((n_blk, blk, HEAD_DIM), F32),
                pltpu.VMEM((n_blk, HEAD_DIM, blk), BF16),
                pltpu.VMEM((n_blk, HEAD_DIM, blk), BF16),
            ],
        ),
        compiler_params=pltpu.CompilerParams(vmem_limit_bytes=63 * 1024 * 1024),
        cost_estimate=pl.CostEstimate(flops=6 * n_heads * tokens * tokens * HEAD_DIM * 2, bytes_accessed=10 * tokens * width, transcendentals=0),
        name="attn_fwd_bwd",
    )(cu_doc, qkv, d_out, qkv, qkv, cos_t, sin_t)


def solution(mesh):
    n_dev = mesh.shape["sp"]
    tok_spec = P(("dp", "sp"), None)
    vec_spec = P(("dp", "sp"))
    rep_spec = P()

    def exchange(parts):
        return lax.all_to_all(parts, "sp", 0, 0, tiled=True)

    def per_device(hidden, pos_ids, cu_doc, grad_y, norm_w, w_q, b_q, w_k, b_k, w_v, b_v, w_o):
        tokens, width = hidden.shape
        me = lax.axis_index("sp")
        q_cols = w_q.shape[1] // n_dev
        kv_cols = w_k.shape[1] // n_dev
        n_heads = q_cols // HEAD_DIM

        h_f32 = hidden.astype(F32)
        inv_rms = lax.rsqrt(jnp.mean(h_f32 * h_f32, axis=-1, keepdims=True) + NORM_EPS)
        normed = h_f32 * inv_rms
        gain = norm_w.astype(F32)
        u_loc = (normed * gain).astype(BF16)
        u_all = lax.all_gather(u_loc, "sp", axis=0, tiled=True)
        pos_all = lax.all_gather(pos_ids, "sp", axis=1, tiled=True)
        cos_t, sin_t = rope_tables(pos_all)

        d_attn = jnp.einsum("td,qd->tq", grad_y, w_o, preferred_element_type=F32).astype(BF16)
        d_parts = d_attn.reshape(tokens, n_dev, q_cols).transpose(1, 0, 2)
        d_parts, u_all, cos_t, sin_t = lax.optimization_barrier((d_parts, u_all, cos_t, sin_t))
        d_out = exchange(d_parts).reshape(n_dev * tokens, q_cols)

        def own(w, cols):
            return lax.dynamic_slice_in_dim(w, me * cols, cols, axis=w.ndim - 1)

        w_cat = jnp.concatenate([own(w_q, q_cols), own(w_k, kv_cols), own(w_v, kv_cols)], axis=1)
        b_cat = jnp.concatenate([own(b_q, q_cols), own(b_k, kv_cols), own(b_v, kv_cols)]).astype(F32)[None, :]
        qkv = project(u_all, w_cat, b_cat, cos_t, sin_t, n_heads + kv_cols // HEAD_DIM)

        gy_src, qkv, d_out = lax.optimization_barrier((grad_y, qkv, d_out))
        gy_all = lax.all_gather(gy_src, "sp", axis=0, tiled=True)

        o_h, gq_h, gk_h, gv_h, gbq, gbk, gbv = attend(cu_doc, qkv, d_out, cos_t, sin_t, n_heads)
        o_h, gq_h, gk_h, gv_h, gy_all = lax.optimization_barrier((o_h, gq_h, gk_h, gv_h, gy_all))

        o_tok = exchange(o_h.reshape(n_dev, tokens, q_cols)).transpose(1, 0, 2).reshape(tokens, n_dev * q_cols)
        gq_tok = exchange(gq_h.reshape(n_dev, tokens, q_cols)).transpose(1, 0, 2).reshape(tokens, n_dev * q_cols)
        gkv_h = jnp.stack([gk_h.reshape(n_dev, tokens, kv_cols), gv_h.reshape(n_dev, tokens, kv_cols)], axis=1)
        gkv_tok = exchange(gkv_h).transpose(1, 2, 0, 3).reshape(2, tokens, n_dev * kv_cols)

        grad_w_o = lax.dot_general(o_h, gy_all, (((0,), (0,)), ((), ())), preferred_element_type=F32)
        g_cat = jnp.concatenate([gq_h, gk_h, gv_h], axis=1)
        gw_cat = lax.dot_general(u_all, g_cat, (((0,), (0,)), ((), ())), preferred_element_type=F32)
        rows = width // n_dev
        gw_got = exchange(gw_cat.reshape(n_dev, rows, q_cols + 2 * kv_cols))

        def columns(lo, size):
            return gw_got[:, :, lo:lo + size].transpose(1, 0, 2).reshape(rows, n_dev * size)

        grad_w_q = columns(0, q_cols)
        grad_w_k = columns(q_cols, kv_cols)
        grad_w_v = columns(q_cols + kv_cols, kv_cols)

        y_out = (h_f32 + jnp.dot(o_tok, w_o, preferred_element_type=F32)).astype(BF16)
        d_norm = dot_t(gq_tok, w_q) + dot_t(gkv_tok[0], w_k) + dot_t(gkv_tok[1], w_v)
        norm_part = jnp.sum(d_norm * normed, axis=0)
        d_scaled = d_norm * gain
        d_hidden = inv_rms * (d_scaled - normed * jnp.mean(d_scaled * normed, axis=-1, keepdims=True))
        grad_hidden = (grad_y.astype(F32) + d_hidden).astype(BF16)
        norm_part, y_out, grad_w_o, grad_hidden, grad_w_q = lax.optimization_barrier((norm_part, y_out, grad_w_o, grad_hidden, grad_w_q))
        grad_norm_w = lax.psum_scatter(norm_part, "sp", scatter_dimension=0, tiled=True)
        return (y_out, grad_hidden, grad_norm_w, grad_w_q, jnp.sum(gbq, axis=0), grad_w_k, jnp.sum(gbk, axis=0), grad_w_v, jnp.sum(gbv, axis=0), grad_w_o)

    in_specs = (tok_spec, P(None, ("dp", "sp")), P("dp"), tok_spec, rep_spec, rep_spec, rep_spec, rep_spec, rep_spec, rep_spec, rep_spec, rep_spec)
    out_specs = (tok_spec, tok_spec, vec_spec, tok_spec, vec_spec, tok_spec, vec_spec, tok_spec, vec_spec, tok_spec)
    return jax.shard_map(per_device, mesh=mesh, in_specs=in_specs, out_specs=out_specs, check_vma=False)
```
